32 devices in a mesh: trial: 4 (over z), ep: 4 (over y, core), fsdp: 2 (over x).
Axes of the slice: x: 2, y: 2, z: 4, core: 2. Of those that a mesh axis runs over, the one named last changes fastest.
Arguments:
- master_down: float32 [256, 1024, 2048], P(('trial', 'ep'), None, 'fsdp'), parts along dimension 0, may hold values from -0.25 to 0.25
- router_weight: float32 [8192, 64], P(('trial', 'fsdp'), 'ep'), parts along dimension 0, may hold values from -0.125 to 0.125
- router_gain: float32 [8192], P(('trial', 'fsdp')), parts along dimension 0, may hold values from 0.25 to 1.75
Outputs:
- final_down: bfloat16 [256, 1024, 2048], P(('trial', 'ep'), 'fsdp'), parts along dimension 0
- scale_down: float32 [256, 1024], P(('trial', 'ep'), 'fsdp'), parts along dimension 0
- serve_router: bfloat16 [8192, 64], P('trial'), parts along dimension 0
The draws below stay inside these ranges and needn't reach their ends.
There are 4 independent parts, one for each index of `trial`. The reference program is written for one: setup_inputs(seed, part) draws one part's arguments, and reference() takes and returns one part's arrays. A program takes and returns all parts, laid end to end along the dimension named above; each array names one. Nothing has to cross between parts.
All inputs are finite; a program needn't handle non-finite values. Where the reference program divides by a largest or mean magnitude, that divisor is 1e-20 or more.
Results may differ from the reference program's by a relative error of at most 0.001.
Values may be sent and summed in bfloat16 or wider, within the bound.
A program may use at most 256 MiB of HBM per device.

```python
import jax
import jax.numpy as jnp

EXPERTS = 64
D_MODEL = 2048
D_EXPERT = 1024


def strengthened(array, key, source, target, shards_of, factor):
    def block_of(position):
        return (jnp.arange(array.shape[position]) // (array.shape[position] // shards_of)).reshape((-1,) + (1,) * (array.ndim - 1 - position))

    first = jax.random.permutation(key, shards_of)[block_of(target)]
    second = (block_of(target) + shards_of // 2) % shards_of
    return jnp.where((block_of(source) == first) | (block_of(source) == second), factor * array, array)


def block_scale(own_key, dims, cuts, smallest, largest):
    level = 1.0
    for axis_at, shards_of in cuts:
        draws = jax.random.uniform(jax.random.fold_in(jax.random.fold_in(own_key, 6), axis_at), (shards_of,), jnp.float32, smallest / len(cuts), largest / len(cuts))
        level = level * jnp.repeat(jnp.exp(draws), dims[axis_at] // shards_of).reshape((-1,) + (1,) * (len(dims) - 1 - axis_at))
    return level


def centred(own_key, shape, scale, bound, pieces=(), kind=jnp.bfloat16):
    result = jax.random.normal(own_key, shape, jnp.float32) * scale
    if len(pieces) > 0:
        result = block_scale(own_key, shape, pieces, -0.22, 0.18) * result
    return jnp.clip(result, min=-bound, max=bound).astype(kind)


def bell_draw_with(rng, extent, deviation, reach, split, heavy, kind=jnp.bfloat16):
    result = deviation * jax.random.normal(rng, extent, jnp.float32)
    if split:
        result = result * block_scale(rng, extent, split, -0.22, 0.18)
    return jnp.clip(strengthened(result, jax.random.fold_in(rng, 3), *heavy), -reach, reach).astype(kind)


def setup_inputs(seed: int = 0, part: int = 0) -> dict:
    arg_keys = jax.random.split(jax.random.key(seed), 4)
    part_splits = jax.random.split(jax.random.fold_in(arg_keys[3], part), 4)
    master_down = bell_draw_with(part_splits[0], (EXPERTS, D_EXPERT, D_MODEL), D_EXPERT ** -0.5, 0.25, ((0, 4), (2, 2)), (2, 1, 2, 2.0), jnp.float32)
    router_weight = centred(part_splits[1], (D_MODEL, EXPERTS), D_MODEL ** -0.5, 0.125, ((0, 2), (1, 4)), jnp.float32)
    router_gain = jnp.clip(1.0 + 0.15 * jax.random.normal(part_splits[2], (D_MODEL,), jnp.float32), 0.25, 1.75)
    return dict(master_down=master_down, router_weight=router_weight, router_gain=router_gain)


def reference(master_down, router_weight, router_gain):
    scale_down = jnp.max(jnp.abs(master_down), axis=2)
    final_down = (master_down / jnp.expand_dims(scale_down, 2)).astype(jnp.bfloat16)
    serve_router = (router_weight * router_gain[:, None]).astype(jnp.bfloat16)
    return final_down, scale_down, serve_router
```

```python
import functools

import jax
import jax.numpy as jnp
from jax import lax
from jax.experimental import pallas as pl
from jax.experimental.pallas import tpu as pltpu
from jax.sharding import PartitionSpec as P


ANY = pl.BlockSpec(memory_space=pl.ANY)


def cost(nbytes):
    return pl.CostEstimate(flops=nbytes, bytes_accessed=nbytes, transcendentals=0)


def maxima_kernel(x_ref, *rest):
    rest[-1][0] = jnp.broadcast_to(jnp.max(jnp.abs(x_ref[0]), axis=1, keepdims=True), (x_ref.shape[1], 128)).T[0:1]


def maxima(master, first, count, after):
    _, rows, cols = master.shape
    part = rows // 4
    return pl.pallas_call(
        maxima_kernel,
        grid=(count, 4),
        in_specs=[pl.BlockSpec((1, part, cols), lambda i, r: (first + i, r, 0))] + [ANY] * len(after),
        out_specs=pl.BlockSpec((1, 1, part), lambda i, r: (i, 0, r)),
        out_shape=jax.ShapeDtypeStruct((count, 1, rows), jnp.float32),
        cost_estimate=cost(count * rows * cols * 4),
    )(master, *after)


def narrowed(x_ref, here_ref, there_ref):
    scale = jnp.maximum(here_ref[0], there_ref[0])
    column = jnp.broadcast_to(scale, (8, scale.shape[1])).T[:, 0:1]
    return (x_ref[0] * (1.0 / column)).astype(jnp.bfloat16), scale


def narrow_kernel(me_ref, x_away, x_home, here_away, there_away, here_home, there_home, *rest):
    send_ref, final_ref, scale_ref = rest[-3:]
    send_ref[0], _ = narrowed(x_away, here_away, there_away)
    final_ref[0], scale_ref[0] = narrowed(x_home, here_home, there_home)


def narrow(me, master, here, there, first, count, at, final, after):
    experts, rows, cols = master.shape
    half, part = rows // 2, rows // 4

    def x_spec(away):
        return pl.BlockSpec((1, part, cols), lambda i, r, m: (first + i, (1 - m[0] if away else m[0]) * 2 + r, 0))

    def m_spec(away):
        return pl.BlockSpec((1, 1, part), lambda i, r, m: (at + i, 0, (1 - m[0] if away else m[0]) * 2 + r))

    extra = ([] if final is None else [final]) + list(after)
    return pl.pallas_call(
        narrow_kernel,
        grid_spec=pltpu.PrefetchScalarGridSpec(
            num_scalar_prefetch=1,
            grid=(count, 2),
            in_specs=[x_spec(True), x_spec(False), m_spec(True), m_spec(True), m_spec(False), m_spec(False)]
            + [ANY] * len(extra),
            out_specs=[
                pl.BlockSpec((1, part, cols), lambda i, r, m: (i, r, 0)),
                pl.BlockSpec((1, part, cols), lambda i, r, m: (first + i, r, m[0])),
                pl.BlockSpec((1, 1, part), lambda i, r, m: (i, 0, r)),
            ],
        ),
        out_shape=[
            jax.ShapeDtypeStruct((count, half, cols), jnp.bfloat16),
            jax.ShapeDtypeStruct((experts, half, 2 * cols), jnp.bfloat16),
            jax.ShapeDtypeStruct((count, 1, half), jnp.float32),
        ],
        input_output_aliases={} if final is None else {7: 1},
        cost_estimate=cost(count * rows * cols * 6),
    )(me, master, master, here, there, here, there, *extra)


def place_kernel(me_ref, came_ref, *rest):
    rest[-1][...] = came_ref[...]


def place(me, came, first, final, after):
    count, half, cols = came.shape
    part = half // 2
    return pl.pallas_call(
        place_kernel,
        grid_spec=pltpu.PrefetchScalarGridSpec(
            num_scalar_prefetch=1,
            grid=(count, 2),
            in_specs=[pl.BlockSpec((1, part, cols), lambda i, r, m: (i, r, 0)), ANY] + [ANY] * len(after),
            out_specs=pl.BlockSpec((1, part, cols), lambda i, r, m: (first + i, r, 1 - m[0])),
        ),
        out_shape=jax.ShapeDtypeStruct(final.shape, final.dtype),
        input_output_aliases={2: 0},
        cost_estimate=cost(count * half * cols * 4),
    )(me, came, final, *after)


def router_kernel(w_ref, g_ref, *rest):
    rest[-1][...] = (w_ref[...] * g_ref[...]).astype(jnp.bfloat16)


def router(weight, gain, after):
    turned, gains = weight.T, gain[None, :]
    return pl.pallas_call(
        router_kernel,
        in_specs=[pl.BlockSpec(turned.shape, lambda: (0, 0)), pl.BlockSpec(gains.shape, lambda: (0, 0))]
        + [ANY] * len(after),
        out_specs=pl.BlockSpec(turned.shape, lambda: (0, 0)),
        out_shape=jax.ShapeDtypeStruct(turned.shape, jnp.bfloat16),
        cost_estimate=cost(turned.size * 6),
    )(turned, gains, *after)


def swap(array):
    return lax.ppermute(array, "fsdp", [(0, 1), (1, 0)])


def pieces(experts):
    middle = max(experts - 4, 0)
    sizes = [1] * min(experts, 2) + [2] * (middle // 2) + [1] * (middle % 2) + [1] * max(min(experts, 4) - 2, 0)
    starts = [sum(sizes[:k]) for k in range(len(sizes))]
    return list(zip(starts, sizes))


def paired_shards(master_down, router_weight, router_gain):
    experts = master_down.shape[0]
    index = lax.axis_index("fsdp")
    me = index.astype(jnp.int32).reshape(1)
    cut = pieces(experts)

    groups = [g for g in (cut[:1], cut[1:3], cut[3:]) if g]
    bounds = [(g[0][0], sum(size for _, size in g)) for g in groups]
    here, there, home = [], [], {}
    for number, (first, count) in enumerate(bounds[:2]):
        here.append(maxima(master_down, first, count, here[-1:]))
        there.append(swap(here[-1]))
    for number, group in enumerate(groups):
        for first, size in group:
            home[first] = (number, first - bounds[number][0])

    final, scales, flying = None, [], []
    gathered = None

    def step(k, after):
        nonlocal final
        first, size = cut[k]
        number, at = home[first]
        send, final, scale = narrow(me, master_down, here[number], there[number], first, size, at, final, after)
        scales.append(scale)
        flying.append(swap(send))

    step(0, here[1:2])
    if len(groups) > 2:
        here.append(maxima(master_down, *bounds[2], scales[-1:]))
        there.append(swap(here[-1]))
    if len(cut) > 1:
        step(1, here[2:3])
    for k in range(len(cut)):
        after = []
        if k == len(cut) - 1:
            scale_down = jnp.concatenate(scales, axis=0).reshape(experts, -1)
            after = [scale_down, serve]
        final = place(me, flying[k], cut[k][0], final, after)
        if k == 0:
            part = router(router_weight, router_gain, [final])
            columns = lax.all_gather(part, "ep", axis=0, tiled=True)
            other = swap(columns)
        if k == len(cut) // 2 or (k == 0 and len(cut) == 1):
            low = jnp.where(index == 0, columns, other)
            high = jnp.where(index == 0, other, columns)
            serve = jnp.concatenate([low, high], axis=1)
        if k + 2 < len(cut):
            step(k + 2, [columns] if k == 0 else [])
    return (final, scale_down, serve.T)


def shards(master_down, router_weight, router_gain):
    scale_down = lax.pmax(jnp.max(jnp.abs(master_down), axis=2), "fsdp")
    narrow_down = (master_down / jnp.expand_dims(scale_down, 2)).astype(jnp.bfloat16)
    final_down = lax.all_to_all(narrow_down, "fsdp", split_axis=1, concat_axis=2, tiled=True)
    scale_down = lax.dynamic_slice_in_dim(
        scale_down, lax.axis_index("fsdp") * final_down.shape[1], final_down.shape[1], axis=1
    )
    part_router = (router_weight * router_gain[:, None]).astype(jnp.bfloat16)
    row_router = lax.all_gather(part_router, "fsdp", axis=0, tiled=True)
    serve_router = lax.all_gather(row_router, "ep", axis=1, tiled=True)
    return (final_down, scale_down, serve_router)


def solution(mesh):
    return jax.shard_map(
        paired_shards if mesh.shape["fsdp"] == 2 else shards,
        mesh=mesh,
        in_specs=(
            P(("trial", "ep"), None, "fsdp"),
            P(("trial", "fsdp"), "ep"),
            P(("trial", "fsdp")),
        ),
        out_specs=(P(("trial", "ep"), "fsdp", None), P(("trial", "ep"), "fsdp"), P("trial", None)),
        check_vma=False,
    )
```
